256 devices in a mesh: groups: 2 (over z), freq: 128 (over x, y, core).
Axes of the slice: x: 8, y: 8, z: 2, core: 2. Of those that a mesh axis runs over, the one named last changes fastest.
The devices are a block of a 8x8x16 slice.
Arguments:
- traces: bfloat16 [1024, 2048, 256], P('freq', None, 'groups'), parts along dimension 2, may hold values from -24 to 24
- freq_index: int32 [128], replicated, may hold values from 1 to 511
- block_map: int32 [64, 64], replicated, may hold values 0 or 1
- green_rec: bfloat16 [128, 2, 2048, 1536], P('freq', None, None, 'groups'), parts along dimension 3, may hold values from -0.5 to 0.5
- green_src: bfloat16 [128, 2, 128, 1536], P('freq', None, None, 'groups'), parts along dimension 3, may hold values from -0.03125 to 0.03125
Outputs:
- image: float32 [1536], P(('groups', 'freq')), parts along dimension 0
The draws below stay inside these ranges and needn't reach their ends.
There are 2 independent parts, one for each index of `groups`. The reference program is written for one: setup_inputs(seed, part) draws one part's arguments, and reference() takes and returns one part's arrays. A program takes and returns all parts, laid end to end along the dimension named above; an argument that names none is the same for every part. Nothing has to cross between parts.
Inputs may be any that keep to these rules, and one draw needn't show every extreme that they name: `freq_index`: frequency bins; they may repeat. `block_map`: 1 where a receiver block lies in an image tile's aperture.
All inputs are finite; a program needn't handle non-finite values.
Results may differ from the reference program's by a relative error of at most 0.0038.
Values may be sent and summed in bfloat16 or wider, within the bound.
A program may use at most 64 MiB of HBM per device.

```python
import math
import jax
import jax.numpy as jnp
from jax import lax

NT = 1024
R = 2048
RBLK = 64
TILES = 64
P_SIZE = 768
S = 128
FREQS = 128


def place_ends(result, key, low, largest):
    extent = result.shape
    spot = [jax.random.randint(jax.random.fold_in(key, axis), (), 0, extent[axis]) for axis in range(len(extent))]
    result = result.at[tuple(spot)].set(low)
    longest = extent.index(max(extent))
    spot[longest] = (spot[longest] + 1) % extent[longest]
    return result.at[tuple(spot)].set(largest)


def strengthened(entries, stream_key, source, target, shards_of, factor):
    owner, partner = [(jnp.arange(entries.shape[axis_at]) // (entries.shape[axis_at] // shards_of)).reshape([-1 if axis == axis_at else 1 for axis in range(entries.ndim)]) for axis_at in (source, target)]
    chosen = jax.random.permutation(stream_key, shards_of)[partner]
    strong = (owner == chosen) | (owner == (partner + shards_of // 2) % shards_of)
    return jnp.where(strong, factor * entries, entries)


def block_levels(key, shape, split, smallest, top_value):
    def one(position, blocks):
        heights = jax.random.uniform(jax.random.fold_in(jax.random.fold_in(key, 6), position), (blocks,), jnp.float32, smallest / len(split), top_value / len(split))
        return jnp.repeat(jnp.exp(heights), shape[position] // blocks).reshape((-1,) + (1,) * (len(shape) - position - 1))

    gain = one(*split[0])
    for cut in split[1:]:
        gain = gain * one(*cut)
    return gain


def centred(key, dims, width, bound, pieces=(), held_as=jnp.bfloat16):
    array = jax.random.normal(key, dims, jnp.float32) * width
    if len(pieces) > 0:
        array = block_levels(key, dims, pieces, -0.22, 0.18) * array
    return jnp.clip(array, min=-bound, max=bound).astype(held_as)


def gaussian_with(rng, extent, width, most, shards, heavy, kind=jnp.bfloat16):
    entries = width * jax.random.normal(rng, extent, jnp.float32)
    if shards:
        entries = entries * block_levels(rng, extent, shards, -0.22, 0.18)
    return jnp.clip(strengthened(entries, jax.random.fold_in(rng, 3), *heavy), -most, most).astype(kind)


def setup_inputs(seed: int = 0, part: int = 0) -> dict:
    key_of = jax.random.split(jax.random.key(seed), 6)
    part_keys = jax.random.split(jax.random.fold_in(key_of[5], part), 6)
    return {
        "traces": gaussian_with(part_keys[0], (NT, R, S), 1.0, 24.0, ((0, 128),), (0, 1, 128, 5.5)),
        "freq_index": place_ends(jax.random.randint(key_of[1], (FREQS,), 1, NT // 2), jax.random.fold_in(key_of[1], 1), 1, (NT // 2) - 1).astype(jnp.int32),
        "block_map": place_ends((jax.random.randint(key_of[2], (RBLK, TILES), 0, 3) < 1).astype(jnp.int32), jax.random.fold_in(key_of[2], 1), 0, 1),
        "green_rec": gaussian_with(part_keys[3], (FREQS, 2, R, P_SIZE), R ** -0.5, 0.5, ((0, 128),), (0, 3, 128, 5.5)),
        "green_src": centred(part_keys[4], (FREQS, 2, S, P_SIZE), (2 * S * FREQS) ** -0.5, 0.03125, ((0, 128),)),
    }


def dft_table(freq_index, length):
    sample_index = jnp.arange(length, dtype=jnp.int32)
    phases = freq_index[:, None] * sample_index[None, :] % length
    angles = phases.astype(jnp.float32) * jnp.float32(2.0 * math.pi / length)
    stacked = jnp.stack((jnp.cos(angles), -jnp.sin(angles)), axis=1)
    return stacked.reshape(freq_index.shape[0] * 2, length).astype(jnp.bfloat16)

def expand_map(block_map, receivers, points):
    row_span = receivers // block_map.shape[0]
    col_span = points // block_map.shape[1]
    return jnp.repeat(jnp.repeat(block_map, row_span, axis=0), col_span, axis=1).astype(jnp.bfloat16)

def reference(traces, freq_index, block_map, green_rec, green_src):
    cos_table = dft_table(freq_index, NT)
    spectrum = jnp.dot(cos_table, traces.reshape(NT, R * S), preferred_element_type=jnp.float32)
    spectrum = (spectrum * (1.0 / math.sqrt(NT))).astype(jnp.bfloat16).reshape(FREQS, 2, R, S)
    mask_full = expand_map(block_map, R, P_SIZE)

    def per_freq(image_sum, stacked):
        spec_f, rec_f, src_f = stacked
        masked = (rec_f * mask_full[None]).astype(jnp.float32)
        spec_w = spec_f.astype(jnp.float32)
        swapped = jnp.stack((spec_w[1], -spec_w[0]), axis=0)
        blocks = jnp.stack((spec_w, swapped), axis=0)
        back_field = jnp.einsum('crx,ocrs->osx', masked, blocks, precision=lax.Precision.HIGHEST)
        image_sum = image_sum + lax.optimization_barrier(jnp.sum(src_f.astype(jnp.float32) * back_field, axis=(0, 1)))
        return (image_sum, None)
    image, _ = lax.scan(per_freq, jnp.zeros((P_SIZE,), jnp.float32), (spectrum, green_rec, green_src))
    return image
```

```python
import functools
import math

import jax
import jax.numpy as jnp
from jax import lax
from jax.experimental import pallas as pl
from jax.experimental.pallas import tpu as pltpu
from jax.sharding import PartitionSpec as P

MESH = pl.DeviceIdType.MESH
BF16, F32 = jnp.bfloat16, jnp.float32
CHUNKS = 2
SUB = 8
LANES = 128


def dft_table(freq_index, length):
    sample_index = jnp.arange(length, dtype=jnp.int32)
    phases = freq_index[:, None] * sample_index[None, :] % length
    angles = phases.astype(jnp.float32) * jnp.float32(2.0 * math.pi / length)
    stacked = jnp.stack((jnp.cos(angles), -jnp.sin(angles)), axis=1)
    return stacked.reshape(freq_index.shape[0] * 2, length).astype(jnp.bfloat16)


def iota(shape, dim):
    return lax.broadcasted_iota(jnp.int32, shape, dim)


def one_hot(pred):
    return jnp.where(pred, 1.0, 0.0).astype(F32)


def swap_matrix(outer, inner):
    size = outer * inner
    row, col = iota((size, size), 0), iota((size, size), 1)
    return one_hot((row // outer == col % inner) & (row % outer == col // inner)).astype(BF16)


def exact_dot(a, b):
    return jnp.dot(a, b, preferred_element_type=F32, precision=lax.Precision.HIGHEST)


def kernel(
    n, traces, table, block_map, green_rec, green_src, out,
    xbuf, xt, yb, spec, pbuf, masked, colmask, src, back, istage, ibuf,
    x_send, x_recv, p_send, p_recv, i_send, i_recv, g_sem, s_sem,
):
    me = lax.axis_index("freq")
    tsub = traces.shape[0]
    length = n * tsub
    receivers = traces.shape[1]
    points = green_rec.shape[2]
    per_chunk = receivers // CHUNKS

    def peer(d):
        return lax.rem(me + d, n)

    load_rec = pltpu.make_async_copy(green_rec, masked, g_sem)
    load_src = pltpu.make_async_copy(green_src, src, s_sem)
    load_rec.start()
    load_src.start()

    barrier = pltpu.get_barrier_semaphore()

    @pl.loop(1, n)
    def _(d):
        pl.semaphore_signal(barrier, inc=1, device_id={"freq": peer(d)}, device_id_type=MESH)

    pl.semaphore_wait(barrier, n - 1)

    for c in range(CHUNKS):
        def block_of(j, c=c):
            start = pl.multiple_of(c * per_chunk + j * SUB, SUB)
            return traces.at[:, pl.ds(start, SUB), :]

        @pl.loop(1, n)
        def _(d, c=c, block_of=block_of):
            j = peer(d)
            pltpu.make_async_remote_copy(
                src_ref=block_of(j), dst_ref=xbuf.at[c, me],
                send_sem=x_send, recv_sem=x_recv.at[c],
                device_id={"freq": j}, device_id_type=MESH,
            ).start()

        pltpu.make_async_copy(block_of(me), xbuf.at[c, me], x_recv.at[c]).start()

    tiles = block_map.shape[1]
    rblk = block_map.shape[0]
    spread = one_hot(iota((tiles, points), 1) // (points // tiles) == iota((tiles, points), 0))
    colmask[...] = jnp.dot(block_map[...].astype(F32), spread, preferred_element_type=F32)
    load_rec.wait()
    load_src.wait()
    span = receivers // rblk

    @pl.loop(0, rblk)
    def _(b):
        row = jnp.broadcast_to(colmask[pl.ds(b, 1), :], (span, points)).astype(BF16)
        rows = pl.ds(pl.multiple_of(b * span, span), span)
        for c in range(2):
            masked[c, rows, :] = masked[c, rows, :] * row

    back[...] = jnp.zeros_like(back)
    tb = 256 // SUB
    kb = tb // tsub
    swap_in = swap_matrix(tb, SUB)
    swap_out = swap_matrix(SUB, tb)
    fcs = table.shape[0]
    scale = 1.0 / math.sqrt(length)

    def transform(c):
        pltpu.make_async_copy(xbuf.at[c], xbuf.at[c], x_recv.at[c]).wait()

        @pl.loop(0, length // tb // 2)
        def _(b):
            both = [
                xbuf[c, pl.ds((2 * b + h) * kb, kb)].reshape(tb * SUB, LANES) for h in range(2)
            ]
            y = jnp.dot(swap_in, jnp.concatenate(both, axis=1), preferred_element_type=F32)
            y = y.astype(BF16).reshape(SUB, tb, 2 * LANES)
            for h in range(2):
                rows = pl.ds(pl.multiple_of((2 * b + h) * tb, tb), tb)
                for r in range(SUB):
                    xt[r // 2, rows, (r % 2) * LANES : (r % 2 + 1) * LANES] = y[
                        r, :, h * LANES : (h + 1) * LANES
                    ]

        for rp in range(SUB // 2):
            o = jnp.dot(table[...], xt[rp], preferred_element_type=F32) * scale
            o = o.astype(BF16)
            yb[2 * rp] = o[:, :LANES]
            yb[2 * rp + 1] = o[:, LANES:]

        for j in range(0, fcs // tb, 2):
            both = [yb[:, (j + h) * tb : (j + h + 1) * tb, :].reshape(256, LANES) for h in range(2)]
            y = jnp.dot(swap_out, jnp.concatenate(both, axis=1), preferred_element_type=F32)
            y = y.astype(BF16)
            for h in range(2):
                spec[c, (j + h) * tb // 2 : (j + h + 1) * tb // 2] = y[
                    :, h * LANES : (h + 1) * LANES
                ].reshape(tb // 2, 2, SUB, LANES)

        @pl.loop(1, n)
        def _(d):
            j = peer(d)
            pltpu.make_async_remote_copy(
                src_ref=spec.at[c, j], dst_ref=pbuf.at[c, me],
                send_sem=p_send, recv_sem=p_recv.at[c],
                device_id={"freq": j}, device_id_type=MESH,
            ).start()

        pbuf[c, me] = spec[c, me]

    def project(c):
        most = pbuf.at[c, pl.ds(0, n - 1)]
        pltpu.make_async_copy(most, most, p_recv.at[c]).wait()
        rows = slice(c * per_chunk, (c + 1) * per_chunk)
        p0 = pbuf[c, :, 0].reshape(per_chunk, LANES)
        p1 = pbuf[c, :, 1].reshape(per_chunk, LANES)
        dims = (((0,), (0,)), ((), ()))
        back[...] += lax.dot_general(
            jnp.concatenate([p0, p1], axis=1), masked[0, rows, :], dims, preferred_element_type=F32
        )
        back[...] += lax.dot_general(
            jnp.concatenate([p1, -p0], axis=1), masked[1, rows, :], dims, preferred_element_type=F32
        )

    for c in range(CHUNKS):
        transform(c)
        if c > 0:
            project(c - 1)
    project(CHUNKS - 1)

    shots = src.shape[1]
    image = jnp.zeros((1, points), F32)
    for o in range(2):
        image += jnp.sum(
            src[o].astype(F32) * back[o * shots : (o + 1) * shots, :], axis=0, keepdims=True
        )
    each = points // n
    mine = one_hot(iota((n, points), 1) // each == iota((n, points), 0)) * image
    fold = one_hot(iota((points, LANES), 0) % each == iota((points, LANES), 1))
    istage[...] = exact_dot(mine, fold).reshape(n, 1, LANES)

    @pl.loop(1, n)
    def _(d):
        j = peer(d)
        pltpu.make_async_remote_copy(
            src_ref=istage.at[j], dst_ref=ibuf.at[me],
            send_sem=i_send, recv_sem=i_recv,
            device_id={"freq": j}, device_id_type=MESH,
        ).start()

    ibuf[me] = istage[me]
    most = ibuf.at[pl.ds(0, n - 1)]
    pltpu.make_async_copy(most, most, i_recv).wait()
    out[...] = jnp.sum(ibuf[...], axis=0)

    for c in range(CHUNKS):
        most = xbuf.at[c, pl.ds(0, n - 1)]
        pltpu.make_async_copy(most, most, x_send).wait()
        most = pbuf.at[c, pl.ds(0, n - 1)]
        pltpu.make_async_copy(most, most, p_send).wait()
    most = ibuf.at[pl.ds(0, n - 1)]
    pltpu.make_async_copy(most, most, i_send).wait()


def body(traces, freq_index, block_map, green_rec, green_src):
    n = lax.axis_size("freq")
    tsub, receivers, shots = traces.shape
    length = tsub * n
    points = green_rec.shape[3]
    fcs = 2 * freq_index.shape[0]
    table = dft_table(freq_index, length)
    per = receivers // CHUNKS
    assert freq_index.shape[0] == n and per == n * SUB and shots == LANES
    any_spec = pl.BlockSpec(memory_space=pl.ANY)
    vmem = pl.BlockSpec(memory_space=pltpu.VMEM)
    dma = pltpu.SemaphoreType.DMA
    out = pl.pallas_call(
        functools.partial(kernel, n),
        out_shape=jax.ShapeDtypeStruct((1, LANES), F32),
        in_specs=[any_spec, vmem, vmem, any_spec, any_spec],
        out_specs=vmem,
        scratch_shapes=[
            pltpu.VMEM((CHUNKS, n, tsub, SUB, LANES), BF16),
            pltpu.VMEM((SUB // 2, length, 2 * LANES), BF16),
            pltpu.VMEM((SUB, fcs, LANES), BF16),
            pltpu.VMEM((CHUNKS, n, 2, SUB, LANES), BF16),
            pltpu.VMEM((CHUNKS, n, 2, SUB, LANES), BF16),
            pltpu.VMEM((2, receivers, points), BF16),
            pltpu.VMEM((block_map.shape[0], points), F32),
            pltpu.VMEM((2, shots, points), BF16),
            pltpu.VMEM((2 * shots, points), F32),
            pltpu.VMEM((n, 1, LANES), F32),
            pltpu.VMEM((n, 1, LANES), F32),
            dma, dma((CHUNKS,)), dma, dma((CHUNKS,)), dma, dma, dma, dma,
        ],
        compiler_params=pltpu.CompilerParams(
            collective_id=0, has_side_effects=True, vmem_limit_bytes=60 * 2**20
        ),
    )(traces, table, block_map, green_rec[0], green_src[0])
    return out[0, : points // n]


def solution(mesh):
    placed = (
        P("freq", None, "groups"),
        P(),
        P(),
        P("freq", None, None, "groups"),
        P("freq", None, None, "groups"),
    )
    return jax.shard_map(
        body, mesh=mesh, in_specs=placed, out_specs=P(("groups", "freq")), check_vma=False
    )
```

```python
import functools
import math

import jax
import jax.numpy as jnp
from jax import lax
from jax.experimental import pallas as pl
from jax.experimental.pallas import tpu as pltpu
from jax.sharding import PartitionSpec as P

MESH = pl.DeviceIdType.MESH
BF16, F32 = jnp.bfloat16, jnp.float32
CHUNKS = 2
SUB = 8
LANES = 128
SIDE, CORES = 8, 2
ORBITS = (SIDE // 2) ** 2 - 1
STRIDE, FIRST = 11, 3
BLOCK = 256
UNROLL = 3


def iota(shape, dim):
    return lax.broadcasted_iota(jnp.int32, shape, dim)


def one_hot(pred):
    return jnp.where(pred, 1.0, 0.0).astype(F32)


def permutation(size, source):
    row, col = iota((size, size), 0), iota((size, size), 1)
    return one_hot(source(row) == col).astype(BF16)


def turned(dx, dy, times):
    for _ in range(times):
        dx, dy = -dy, dx
    return dx, dy


def each_peer(me, send):
    core, y, x = me & (CORES - 1), (me // CORES) & (SIDE - 1), me // (CORES * SIDE)

    def at(dx, dy, dc):
        chip = ((x + dx) & (SIDE - 1)) * SIDE + ((y + dy) & (SIDE - 1))
        return chip * CORES + ((core + dc) & (CORES - 1))

    half = SIDE // 2

    @pl.loop(0, ORBITS * CORES, unroll=UNROLL)
    def _(i):
        e = (i * STRIDE + FIRST) % (ORBITS * CORES)
        k, dc = e // CORES, e & (CORES - 1)
        a, b = 1 + (k & (half - 1)), (k // half + 1) & (half - 1)
        for times in range(4):
            dx, dy = turned(a, b, times)
            send(at(dx, dy, dc))

    for dx, dy in ((half, 0), (0, half), (half, half)):
        for dc in range(CORES):
            send(at(dx, dy, dc))
    for dc in range(1, CORES):
        send(at(0, 0, dc))


def exact_dot(a, b):
    return jnp.dot(a, b, preferred_element_type=F32, precision=lax.Precision.HIGHEST)


def kernel(
    n, traces, freq_index, block_map, green_rec, green_src, out,
    table, xbuf, xt, yb, spec, pbuf, masked, colmask, src, back, istage, ibuf,
    x_send, x_recv, p_send, p_recv, i_send, i_recv, g_sem, s_sem,
):
    me = lax.axis_index("freq")
    tsub, receivers, _ = traces.shape
    length = n * tsub
    points = green_rec.shape[2]
    per_chunk = receivers // CHUNKS

    barrier = pltpu.get_barrier_semaphore()

    def greet(j):
        pl.semaphore_signal(barrier, inc=1, device_id={"freq": j}, device_id_type=MESH)

    each_peer(me, greet)

    load_rec = pltpu.make_async_copy(green_rec, masked, g_sem)
    load_src = pltpu.make_async_copy(green_src, src, s_sem)

    def block_of(c, j):
        start = pl.multiple_of(c * per_chunk + j * SUB, SUB)
        return traces.at[:, pl.ds(start, SUB), :]

    own = [
        pltpu.make_async_copy(block_of(c, me), xbuf.at[c, me], x_recv.at[c]) for c in range(CHUNKS)
    ]
    for copy in [*own, load_rec, load_src]:
        copy.start()

    with jax.named_scope("barrier"):
        pl.semaphore_wait(barrier, n - 1)

    with jax.named_scope("send"):
        for c in range(CHUNKS):
            def send_block(j, c=c):
                pltpu.make_async_remote_copy(
                    src_ref=block_of(c, j), dst_ref=xbuf.at[c, me],
                    send_sem=x_send, recv_sem=x_recv.at[c],
                    device_id={"freq": j}, device_id_type=MESH,
                ).start()

            each_peer(me, send_block)

    with jax.named_scope("table"):
        freqs = freq_index.shape[1]
        diagonal = iota((freqs, freqs), 0) == iota((freqs, freqs), 1)
        column = jnp.sum(
            jnp.where(diagonal, freq_index[...].astype(F32), 0.0), axis=1, keepdims=True
        ).astype(jnp.int32)
        phases = lax.rem(column * iota((freqs, length), 1), length)
        angles = phases.astype(F32) * jnp.float32(2.0 * math.pi / length)
        table[:freqs] = jnp.cos(angles).astype(BF16)
        table[freqs:] = (-jnp.sin(angles)).astype(BF16)

    with jax.named_scope("mask"):
        rblk, tiles = block_map.shape
        spread = one_hot(iota((tiles, points), 1) // (points // tiles) == iota((tiles, points), 0))
        colmask[...] = jnp.dot(block_map[...].astype(F32), spread, preferred_element_type=F32)
        load_rec.wait()
        load_src.wait()
        span = receivers // rblk

        @pl.loop(0, rblk, unroll=2)
        def _(b):
            row = jnp.broadcast_to(colmask[pl.ds(b, 1), :], (span, points)).astype(BF16)
            rows = pl.ds(pl.multiple_of(b * span, span), span)
            for c in range(2):
                masked[c, rows, :] = masked[c, rows, :] * row

    tb = BLOCK // SUB
    fb = tb // 2
    kb = tb // tsub
    swap_in = permutation(BLOCK, lambda row: row % tb * SUB + row // tb)
    swap_out = permutation(
        BLOCK, lambda row: row % SUB * tb + row // SUB % 2 * fb + row // (2 * SUB)
    )
    scale = 1.0 / math.sqrt(length)
    back[...] = jnp.zeros_like(back)

    def transform(c):
        with jax.named_scope(f"wait_x{c}"):
            pltpu.make_async_copy(xbuf.at[c], xbuf.at[c], x_recv.at[c]).wait()

        with jax.named_scope(f"swap_in{c}"):
            @pl.loop(0, length // tb // 2, unroll=4)
            def _(b):
                both = [
                    xbuf[c, pl.ds((2 * b + h) * kb, kb)].reshape(BLOCK, LANES) for h in range(2)
                ]
                y = jnp.dot(swap_in, jnp.concatenate(both, axis=1), preferred_element_type=F32)
                y = y.astype(BF16).reshape(SUB, tb, 2 * LANES)
                for h in range(2):
                    rows = pl.ds(pl.multiple_of((2 * b + h) * tb, tb), tb)
                    for r in range(SUB):
                        xt[r // 2, rows, (r % 2) * LANES : (r % 2 + 1) * LANES] = y[
                            r, :, h * LANES : (h + 1) * LANES
                        ]

        with jax.named_scope(f"dft{c}"):
            for rp in range(SUB // 2):
                o = jnp.dot(table[...], xt[rp], preferred_element_type=F32) * scale
                o = o.astype(BF16)
                yb[2 * rp] = o[:, :LANES]
                yb[2 * rp + 1] = o[:, LANES:]

        with jax.named_scope(f"swap_out{c}"):
            def gathered(f0):
                parts = [yb[:, p * freqs + f0 : p * freqs + f0 + fb, :] for p in range(2)]
                return jnp.concatenate(parts, axis=1).reshape(BLOCK, LANES)

            for f0 in range(0, freqs, 2 * fb):
                both = [gathered(f0 + h * fb) for h in range(2)]
                y = jnp.dot(swap_out, jnp.concatenate(both, axis=1), preferred_element_type=F32)
                y = y.astype(BF16)
                for h in range(2):
                    spec[c, f0 + h * fb : f0 + (h + 1) * fb] = y[
                        :, h * LANES : (h + 1) * LANES
                    ].reshape(fb, 2, SUB, LANES)

        with jax.named_scope(f"scatter{c}"):
            def send_spectrum(j):
                pltpu.make_async_remote_copy(
                    src_ref=spec.at[c, j], dst_ref=pbuf.at[c, me],
                    send_sem=p_send, recv_sem=p_recv.at[c],
                    device_id={"freq": j}, device_id_type=MESH,
                ).start()

            each_peer(me, send_spectrum)
            pbuf[c, me] = spec[c, me]

    def project(c):
        with jax.named_scope(f"wait_p{c}"):
            most = pbuf.at[c, pl.ds(0, n - 1)]
            pltpu.make_async_copy(most, most, p_recv.at[c]).wait()
        with jax.named_scope(f"project{c}"):
            rows = slice(c * per_chunk, (c + 1) * per_chunk)
            p0 = pbuf[c, :, 0].reshape(per_chunk, LANES)
            p1 = pbuf[c, :, 1].reshape(per_chunk, LANES)
            dims = (((0,), (0,)), ((), ()))
            back[...] += lax.dot_general(
                jnp.concatenate([p0, p1], axis=1), masked[0, rows, :], dims,
                preferred_element_type=F32,
            )
            back[...] += lax.dot_general(
                jnp.concatenate([p1, -p0], axis=1), masked[1, rows, :], dims,
                preferred_element_type=F32,
            )

    for c in range(CHUNKS):
        transform(c)
        if c > 0:
            project(c - 1)
    project(CHUNKS - 1)

    with jax.named_scope("image"):
        shots = src.shape[1]
        image = jnp.zeros((1, points), F32)
        for o in range(2):
            image += jnp.sum(
                src[o].astype(F32) * back[o * shots : (o + 1) * shots, :], axis=0, keepdims=True
            )
        each = points // n
        mine = one_hot(iota((n, points), 1) // each == iota((n, points), 0)) * image
        fold = one_hot(iota((points, LANES), 0) % each == iota((points, LANES), 1))
        istage[...] = exact_dot(mine, fold).reshape(n, 1, LANES)

    with jax.named_scope("reduce"):
        def send_image(j):
            pltpu.make_async_remote_copy(
                src_ref=istage.at[j], dst_ref=ibuf.at[me],
                send_sem=i_send, recv_sem=i_recv,
                device_id={"freq": j}, device_id_type=MESH,
            ).start()

        each_peer(me, send_image)
        ibuf[me] = istage[me]
    with jax.named_scope("wait_i"):
        most = ibuf.at[pl.ds(0, n - 1)]
        pltpu.make_async_copy(most, most, i_recv).wait()
    with jax.named_scope("last"):
        out[...] = jnp.sum(ibuf[...], axis=0)[:, : points // n]

        for c in range(CHUNKS):
            most = xbuf.at[c, pl.ds(0, n - 1)]
            pltpu.make_async_copy(most, most, x_send).wait()
            most = pbuf.at[c, pl.ds(0, n - 1)]
            pltpu.make_async_copy(most, most, p_send).wait()
        most = ibuf.at[pl.ds(0, n - 1)]
        pltpu.make_async_copy(most, most, i_send).wait()


def body(traces, freq_index, block_map, green_rec, green_src):
    n = lax.axis_size("freq")
    tsub, receivers, shots = traces.shape
    length = tsub * n
    points = green_rec.shape[3]
    fcs = 2 * freq_index.shape[0]
    per = receivers // CHUNKS
    assert freq_index.shape[0] == n == SIDE * SIDE * CORES and per == n * SUB and shots == LANES
    any_spec = pl.BlockSpec(memory_space=pl.ANY)
    vmem = pl.BlockSpec(memory_space=pltpu.VMEM)
    dma = pltpu.SemaphoreType.DMA
    out = pl.pallas_call(
        functools.partial(kernel, n),
        out_shape=jax.ShapeDtypeStruct((1, points // n), F32),
        in_specs=[any_spec, vmem, vmem, any_spec, any_spec],
        out_specs=vmem,
        scratch_shapes=[
            pltpu.VMEM((fcs, length), BF16),
            pltpu.VMEM((CHUNKS, n, tsub, SUB, LANES), BF16),
            pltpu.VMEM((SUB // 2, length, 2 * LANES), BF16),
            pltpu.VMEM((SUB, fcs, LANES), BF16),
            pltpu.VMEM((CHUNKS, n, 2, SUB, LANES), BF16),
            pltpu.VMEM((CHUNKS, n, 2, SUB, LANES), BF16),
            pltpu.VMEM((2, receivers, points), BF16),
            pltpu.VMEM((block_map.shape[0], points), F32),
            pltpu.VMEM((2, shots, points), BF16),
            pltpu.VMEM((2 * shots, points), F32),
            pltpu.VMEM((n, 1, LANES), F32),
            pltpu.VMEM((n, 1, LANES), F32),
            dma, dma((CHUNKS,)), dma, dma((CHUNKS,)), dma, dma, dma, dma,
        ],
        compiler_params=pltpu.CompilerParams(
            collective_id=0, has_side_effects=True, vmem_limit_bytes=60 * 2**20
        ),
    )(traces, freq_index[None], block_map, green_rec[0], green_src[0])
    return out[0]


def solution(mesh):
    placed = (
        P("freq", None, "groups"),
        P(),
        P(),
        P("freq", None, None, "groups"),
        P("freq", None, None, "groups"),
    )
    return jax.shard_map(
        body, mesh=mesh, in_specs=placed, out_specs=P(("groups", "freq")), check_vma=False
    )
```

```python
import functools
import math

import jax
import jax.numpy as jnp
from jax import lax
from jax.experimental import pallas as pl
from jax.experimental.pallas import tpu as pltpu
from jax.sharding import PartitionSpec as P

MESH = pl.DeviceIdType.MESH
BF16, F32 = jnp.bfloat16, jnp.float32
CHUNKS = 2
SUB = 8
LANES = 128
SIDE, CORES = 8, 2
STEPS = ((SIDE // 2) ** 2 - 1) * CORES
MIXED = (23, 3)
FAR_FIRST = (STEPS - 1, 23)
BLOCK = 256
ROOT, AIDE = 0, 1
UNROLL = 3


def iota(shape, dim):
    return lax.broadcasted_iota(jnp.int32, shape, dim)


def one_hot(pred):
    return jnp.where(pred, 1.0, 0.0).astype(F32)


def permutation(size, source):
    row, col = iota((size, size), 0), iota((size, size), 1)
    return one_hot(source(row) == col).astype(BF16)


def turned(dx, dy, times):
    for _ in range(times):
        dx, dy = -dy, dx
    return dx, dy


class Peers:
    def __init__(self, me):
        self.core, self.y, self.x = me & (CORES - 1), (me // CORES) & (SIDE - 1), me // (CORES * SIDE)

    def at(self, dx, dy, dc):
        chip = ((self.x + dx) & (SIDE - 1)) * SIDE + ((self.y + dy) & (SIDE - 1))
        return chip * CORES + ((self.core + dc) & (CORES - 1))

    def opposite(self, send):
        half = SIDE // 2
        for dx, dy in ((half, half), (half, 0), (0, half)):
            for dc in range(CORES):
                send(self.at(dx, dy, dc))

    def turns(self, i, order, send):
        half = SIDE // 2
        stride, first = order
        e = (i * stride + first) % STEPS
        k, dc = e // CORES, e & (CORES - 1)
        a, b = 1 + (k & (half - 1)), (k // half + 1) & (half - 1)
        for times in range(4):
            dx, dy = turned(a, b, times)
            send(self.at(dx, dy, dc))

    def partner(self, send):
        for dc in range(1, CORES):
            send(self.at(0, 0, dc))

    def each(self, order, send):
        self.opposite(send)

        @pl.loop(0, STEPS, unroll=UNROLL)
        def _(i):
            self.turns(i, order, send)

        self.partner(send)


def exact_dot(a, b):
    return jnp.dot(a, b, preferred_element_type=F32, precision=lax.Precision.HIGHEST)


def kernel(
    n, traces, freq_hbm, map_hbm, green_rec, green_src, out,
    freq_index, block_map, table, xbuf, xt, yb, spec, pbuf, masked, colmask, src, back, istage, ibuf,
    x_send, x_recv, p_send, p_recv, i_send, i_recv, g_sem, s_sem, f_sem, m_sem, ready, root_in,
):
    me = lax.axis_index("freq")
    tsub, receivers, _ = traces.shape
    length = n * tsub
    points = green_rec.shape[2]
    per_chunk = receivers // CHUNKS

    barrier = pltpu.get_barrier_semaphore()

    def greet(j):
        pl.semaphore_signal(barrier, inc=1, device_id={"freq": j}, device_id_type=MESH)

    peers = Peers(me)

    @pl.when(me == ROOT)
    def _():
        greet(AIDE)

    @pl.when(me != ROOT)
    def _():
        peers.each(FAR_FIRST, lambda j: pl.when(j > AIDE)(lambda: greet(j)))

    load_rec = pltpu.make_async_copy(green_rec, masked, g_sem)
    load_src = pltpu.make_async_copy(green_src, src, s_sem)

    def block_of(c, j):
        start = pl.multiple_of(c * per_chunk + j * SUB, SUB)
        return traces.at[:, pl.ds(start, SUB), :]

    own = [
        pltpu.make_async_copy(block_of(c, me), xbuf.at[c, me], x_recv.at[c]) for c in range(CHUNKS)
    ]
    small = [
        pltpu.make_async_copy(freq_hbm, freq_index, f_sem),
        pltpu.make_async_copy(map_hbm, block_map, m_sem),
    ]
    for copy in [*own, *small, load_rec, load_src]:
        copy.start()

    def tell(semaphore, j):
        pl.semaphore_signal(semaphore, inc=1, device_id={"freq": j}, device_id_type=MESH)

    with jax.named_scope("barrier"):
        @pl.when(me > AIDE)
        def _():
            pl.semaphore_wait(barrier, n - 2)

        @pl.when(me == AIDE + 1)
        def _():
            tell(ready, AIDE)

        @pl.when(me <= AIDE)
        def _():
            pl.semaphore_wait(ready, 1)

    def send_block(c, j):
        pltpu.make_async_remote_copy(
            src_ref=block_of(c, j), dst_ref=xbuf.at[c, me],
            send_sem=x_send, recv_sem=x_recv.at[c],
            device_id={"freq": j}, device_id_type=MESH,
        ).start()

    def early(j):
        pl.when(j != ROOT)(lambda: send_block(0, j))

    def late(j):
        pl.when(j == ROOT)(lambda: send_block(0, j))

    split = STEPS // 2
    with jax.named_scope("send_early"):
        peers.opposite(early)

        @pl.loop(0, split, unroll=UNROLL)
        def _(i):
            peers.turns(i, MIXED, early)

    with jax.named_scope("root"):
        @pl.when(me == AIDE)
        def _():
            pl.semaphore_wait(barrier, 1)
            tell(ready, ROOT)
            peers.each(FAR_FIRST, lambda j: pl.when(j != ROOT)(lambda: tell(root_in, j)))

        @pl.when(me > AIDE)
        def _():
            pl.semaphore_wait(root_in, 1)

    with jax.named_scope("send"):
        peers.opposite(late)

        @pl.loop(split, STEPS, unroll=UNROLL)
        def _(i):
            peers.turns(i - split, MIXED, late)
            peers.turns(i, MIXED, lambda j: send_block(0, j))

        peers.partner(lambda j: send_block(0, j))
        for c in range(1, CHUNKS):
            peers.each(MIXED, lambda j, c=c: send_block(c, j))

    with jax.named_scope("table"):
        for copy in small:
            copy.wait()
        freqs = freq_index.shape[1]
        diagonal = iota((freqs, freqs), 0) == iota((freqs, freqs), 1)
        column = jnp.sum(
            jnp.where(diagonal, freq_index[...].astype(F32), 0.0), axis=1, keepdims=True
        ).astype(jnp.int32)
        phases = lax.rem(column * iota((freqs, length), 1), length)
        angles = phases.astype(F32) * jnp.float32(2.0 * math.pi / length)
        table[:freqs] = jnp.cos(angles).astype(BF16)
        table[freqs:] = (-jnp.sin(angles)).astype(BF16)

    with jax.named_scope("mask"):
        rblk, tiles = block_map.shape
        spread = one_hot(iota((tiles, points), 1) // (points // tiles) == iota((tiles, points), 0))
        colmask[...] = jnp.dot(block_map[...].astype(F32), spread, preferred_element_type=F32)
        load_rec.wait()
        load_src.wait()
        span = receivers // rblk

        @pl.loop(0, rblk, unroll=2)
        def _(b):
            row = jnp.broadcast_to(colmask[pl.ds(b, 1), :], (span, points)).astype(BF16)
            rows = pl.ds(pl.multiple_of(b * span, span), span)
            for c in range(2):
                masked[c, rows, :] = masked[c, rows, :] * row

    tb = BLOCK // SUB
    fb = tb // 2
    kb = tb // tsub
    swap_in = permutation(BLOCK, lambda row: row % tb * SUB + row // tb)
    swap_out = permutation(
        BLOCK, lambda row: row % SUB * tb + row // SUB % 2 * fb + row // (2 * SUB)
    )
    scale = 1.0 / math.sqrt(length)
    back[...] = jnp.zeros_like(back)

    def transform(c):
        with jax.named_scope(f"wait_x{c}"):
            pltpu.make_async_copy(xbuf.at[c], xbuf.at[c], x_recv.at[c]).wait()

        with jax.named_scope(f"swap_in{c}"):
            @pl.loop(0, length // tb // 2, unroll=4)
            def _(b):
                both = [
                    xbuf[c, pl.ds((2 * b + h) * kb, kb)].reshape(BLOCK, LANES) for h in range(2)
                ]
                y = jnp.dot(swap_in, jnp.concatenate(both, axis=1), preferred_element_type=F32)
                y = y.astype(BF16).reshape(SUB, tb, 2 * LANES)
                for h in range(2):
                    rows = pl.ds(pl.multiple_of((2 * b + h) * tb, tb), tb)
                    for r in range(SUB):
                        xt[r // 2, rows, (r % 2) * LANES : (r % 2 + 1) * LANES] = y[
                            r, :, h * LANES : (h + 1) * LANES
                        ]

        with jax.named_scope(f"dft{c}"):
            for rp in range(SUB // 2):
                o = jnp.dot(table[...], xt[rp], preferred_element_type=F32) * scale
                o = o.astype(BF16)
                yb[2 * rp] = o[:, :LANES]
                yb[2 * rp + 1] = o[:, LANES:]

        with jax.named_scope(f"swap_out{c}"):
            def gathered(f0):
                parts = [yb[:, p * freqs + f0 : p * freqs + f0 + fb, :] for p in range(2)]
                return jnp.concatenate(parts, axis=1).reshape(BLOCK, LANES)

            for f0 in range(0, freqs, 2 * fb):
                both = [gathered(f0 + h * fb) for h in range(2)]
                y = jnp.dot(swap_out, jnp.concatenate(both, axis=1), preferred_element_type=F32)
                y = y.astype(BF16)
                for h in range(2):
                    spec[c, f0 + h * fb : f0 + (h + 1) * fb] = y[
                        :, h * LANES : (h + 1) * LANES
                    ].reshape(fb, 2, SUB, LANES)

        with jax.named_scope(f"scatter{c}"):
            def send_spectrum(j):
                pltpu.make_async_remote_copy(
                    src_ref=spec.at[c, j], dst_ref=pbuf.at[c, me],
                    send_sem=p_send, recv_sem=p_recv.at[c],
                    device_id={"freq": j}, device_id_type=MESH,
                ).start()

            peers.each(MIXED, send_spectrum)
            pbuf[c, me] = spec[c, me]

    def project(c):
        with jax.named_scope(f"wait_p{c}"):
            most = pbuf.at[c, pl.ds(0, n - 1)]
            pltpu.make_async_copy(most, most, p_recv.at[c]).wait()
        with jax.named_scope(f"project{c}"):
            rows = slice(c * per_chunk, (c + 1) * per_chunk)
            p0 = pbuf[c, :, 0].reshape(per_chunk, LANES)
            p1 = pbuf[c, :, 1].reshape(per_chunk, LANES)
            dims = (((0,), (0,)), ((), ()))
            back[...] += lax.dot_general(
                jnp.concatenate([p0, p1], axis=1), masked[0, rows, :], dims,
                preferred_element_type=F32,
            )
            back[...] += lax.dot_general(
                jnp.concatenate([p1, -p0], axis=1), masked[1, rows, :], dims,
                preferred_element_type=F32,
            )

    for c in range(CHUNKS):
        transform(c)
        if c > 0:
            project(c - 1)
    project(CHUNKS - 1)

    with jax.named_scope("image"):
        shots = src.shape[1]
        image = jnp.zeros((1, points), F32)
        for o in range(2):
            image += jnp.sum(
                src[o].astype(F32) * back[o * shots : (o + 1) * shots, :], axis=0, keepdims=True
            )
        each = points // n
        mine = one_hot(iota((n, points), 1) // each == iota((n, points), 0)) * image
        fold = one_hot(iota((points, LANES), 0) % each == iota((points, LANES), 1))
        istage[...] = exact_dot(mine, fold).reshape(n, 1, LANES)

    with jax.named_scope("reduce"):
        def send_image(j):
            pltpu.make_async_remote_copy(
                src_ref=istage.at[j], dst_ref=ibuf.at[me],
                send_sem=i_send, recv_sem=i_recv,
                device_id={"freq": j}, device_id_type=MESH,
            ).start()

        peers.each(FAR_FIRST, send_image)
        ibuf[me] = istage[me]
    with jax.named_scope("wait_i"):
        most = ibuf.at[pl.ds(0, n - 1)]
        pltpu.make_async_copy(most, most, i_recv).wait()
    with jax.named_scope("last"):
        out[...] = jnp.sum(ibuf[...], axis=0)[:, : points // n]

        for c in range(CHUNKS):
            most = xbuf.at[c, pl.ds(0, n - 1)]
            pltpu.make_async_copy(most, most, x_send).wait()
            most = pbuf.at[c, pl.ds(0, n - 1)]
            pltpu.make_async_copy(most, most, p_send).wait()
        most = ibuf.at[pl.ds(0, n - 1)]
        pltpu.make_async_copy(most, most, i_send).wait()


def body(traces, freq_index, block_map, green_rec, green_src):
    n = lax.axis_size("freq")
    tsub, receivers, shots = traces.shape
    length = tsub * n
    points = green_rec.shape[3]
    fcs = 2 * freq_index.shape[0]
    per = receivers // CHUNKS
    assert freq_index.shape[0] == n == SIDE * SIDE * CORES and per == n * SUB and shots == LANES
    any_spec = pl.BlockSpec(memory_space=pl.ANY)
    vmem = pl.BlockSpec(memory_space=pltpu.VMEM)
    dma = pltpu.SemaphoreType.DMA
    out = pl.pallas_call(
        functools.partial(kernel, n),
        out_shape=jax.ShapeDtypeStruct((1, points // n), F32),
        in_specs=[any_spec] * 5,
        out_specs=vmem,
        scratch_shapes=[
            pltpu.VMEM((1, n), jnp.int32),
            pltpu.VMEM(block_map.shape, jnp.int32),
            pltpu.VMEM((fcs, length), BF16),
            pltpu.VMEM((CHUNKS, n, tsub, SUB, LANES), BF16),
            pltpu.VMEM((SUB // 2, length, 2 * LANES), BF16),
            pltpu.VMEM((SUB, fcs, LANES), BF16),
            pltpu.VMEM((CHUNKS, n, 2, SUB, LANES), BF16),
            pltpu.VMEM((CHUNKS, n, 2, SUB, LANES), BF16),
            pltpu.VMEM((2, receivers, points), BF16),
            pltpu.VMEM((block_map.shape[0], points), F32),
            pltpu.VMEM((2, shots, points), BF16),
            pltpu.VMEM((2 * shots, points), F32),
            pltpu.VMEM((n, 1, LANES), F32),
            pltpu.VMEM((n, 1, LANES), F32),
            dma, dma((CHUNKS,)), dma, dma((CHUNKS,)), dma, dma, dma, dma, dma, dma,
            pltpu.SemaphoreType.REGULAR, pltpu.SemaphoreType.REGULAR,
        ],
        compiler_params=pltpu.CompilerParams(
            collective_id=0, has_side_effects=True, vmem_limit_bytes=60 * 2**20
        ),
    )(traces, freq_index[None], block_map, green_rec[0], green_src[0])
    return out[0]


def solution(mesh):
    placed = (
        P("freq", None, "groups"),
        P(),
        P(),
        P("freq", None, None, "groups"),
        P("freq", None, None, "groups"),
    )
    return jax.shard_map(
        body, mesh=mesh, in_specs=placed, out_specs=P(("groups", "freq")), check_vma=False
    )
```

```python
import functools
import math

import jax
import jax.numpy as jnp
from jax import lax
from jax.experimental import pallas as pl
from jax.experimental.pallas import tpu as pltpu
from jax.sharding import PartitionSpec as P

MESH = pl.DeviceIdType.MESH
BF16, F32 = jnp.bfloat16, jnp.float32
CHUNKS = 2
SUB = 8
LANES = 128
SIDE, CORES = 8, 2
STEPS = ((SIDE // 2) ** 2 - 1) * CORES
MIXED = ((17, 8), (19, 23))
FAR_FIRST = (STEPS - 1, 23)
BLOCK = 256
ROOT, AIDE = 0, 1
UNROLL = 3


def iota(shape, dim):
    return lax.broadcasted_iota(jnp.int32, shape, dim)


def one_hot(pred):
    return jnp.where(pred, 1.0, 0.0).astype(F32)


def permutation(size, source):
    row, col = iota((size, size), 0), iota((size, size), 1)
    return one_hot(source(row) == col).astype(BF16)


def turned(dx, dy, times):
    for _ in range(times):
        dx, dy = -dy, dx
    return dx, dy


class Peers:
    def __init__(self, me):
        self.core, self.y, self.x = me & (CORES - 1), (me // CORES) & (SIDE - 1), me // (CORES * SIDE)

    def at(self, dx, dy, dc):
        chip = ((self.x + dx) & (SIDE - 1)) * SIDE + ((self.y + dy) & (SIDE - 1))
        return chip * CORES + ((self.core + dc) & (CORES - 1))

    def opposite(self, send):
        half = SIDE // 2
        for dx, dy in ((half, half), (half, 0), (0, half)):
            for dc in range(CORES):
                send(self.at(dx, dy, dc))

    def turns(self, i, order, send):
        half = SIDE // 2
        stride, first = order
        e = (i * stride + first) % STEPS
        k, dc = e // CORES, e & (CORES - 1)
        a, b = 1 + (k & (half - 1)), (k // half + 1) & (half - 1)
        for times in range(4):
            dx, dy = turned(a, b, times)
            send(self.at(dx, dy, dc))

    def partner(self, send):
        for dc in range(1, CORES):
            send(self.at(0, 0, dc))

    def each(self, order, send):
        self.opposite(send)

        @pl.loop(0, STEPS, unroll=UNROLL)
        def _(i):
            self.turns(i, order, send)

        self.partner(send)


def three_parts(a):
    parts = []
    for _ in range(3):
        parts.append(a.astype(BF16))
        a = a - parts[-1].astype(F32)
    return parts


def kernel(
    n, traces, freq_hbm, map_hbm, green_rec, green_src, out,
    freq_index, block_map, table, xbuf, xt, yb, spec, pbuf, masked, colmask, src, back, pick, fold, istage, ibuf,
    x_send, x_recv, p_send, p_recv, i_send, i_recv, g_sem, s_sem, f_sem, m_sem, ready, root_in,
):
    me = lax.axis_index("freq")
    tsub, receivers, _ = traces.shape
    length = n * tsub
    points = green_rec.shape[2]
    per_chunk = receivers // CHUNKS

    barrier = pltpu.get_barrier_semaphore()

    def greet(j):
        pl.semaphore_signal(barrier, inc=1, device_id={"freq": j}, device_id_type=MESH)

    peers = Peers(me)

    @pl.when(me == ROOT)
    def _():
        greet(AIDE)

    @pl.when(me != ROOT)
    def _():
        peers.each(FAR_FIRST, lambda j: pl.when(j > AIDE)(lambda: greet(j)))

    load_rec = pltpu.make_async_copy(green_rec, masked, g_sem)
    load_src = pltpu.make_async_copy(green_src, src, s_sem)

    def block_of(c, j):
        start = pl.multiple_of(c * per_chunk + j * SUB, SUB)
        return traces.at[:, pl.ds(start, SUB), :]

    own = [
        pltpu.make_async_copy(block_of(c, me), xbuf.at[c, me], x_recv.at[c]) for c in range(CHUNKS)
    ]
    small = [
        pltpu.make_async_copy(freq_hbm, freq_index, f_sem),
        pltpu.make_async_copy(map_hbm, block_map, m_sem),
    ]
    for copy in [*own, *small, load_rec, load_src]:
        copy.start()

    def tell(semaphore, j):
        pl.semaphore_signal(semaphore, inc=1, device_id={"freq": j}, device_id_type=MESH)

    with jax.named_scope("barrier"):
        @pl.when(me > AIDE)
        def _():
            pl.semaphore_wait(barrier, n - 2)

        @pl.when(me == AIDE + 1)
        def _():
            tell(ready, AIDE)

        @pl.when(me <= AIDE)
        def _():
            pl.semaphore_wait(ready, 1)

    def send_block(c, j):
        pltpu.make_async_remote_copy(
            src_ref=block_of(c, j), dst_ref=xbuf.at[c, me],
            send_sem=x_send, recv_sem=x_recv.at[c],
            device_id={"freq": j}, device_id_type=MESH,
        ).start()

    def early(j):
        pl.when(j != ROOT)(lambda: send_block(0, j))

    def late(j):
        pl.when(j == ROOT)(lambda: send_block(0, j))

    split = STEPS // 2
    with jax.named_scope("send_early"):
        peers.opposite(early)

        @pl.loop(0, split, unroll=UNROLL)
        def _(i):
            peers.turns(i, MIXED[0], early)

    with jax.named_scope("root"):
        @pl.when(me == AIDE)
        def _():
            pl.semaphore_wait(barrier, 1)
            tell(ready, ROOT)
            peers.each(FAR_FIRST, lambda j: pl.when(j != ROOT)(lambda: tell(root_in, j)))

        @pl.when(me > AIDE)
        def _():
            pl.semaphore_wait(root_in, 1)

    with jax.named_scope("send"):
        peers.opposite(late)

        @pl.loop(split, STEPS, unroll=UNROLL)
        def _(i):
            peers.turns(i - split, MIXED[0], late)
            peers.turns(i, MIXED[0], lambda j: send_block(0, j))

        peers.partner(lambda j: send_block(0, j))
        for c in range(1, CHUNKS):
            peers.each(MIXED[c], lambda j, c=c: send_block(c, j))

    with jax.named_scope("table"):
        for copy in small:
            copy.wait()
        freqs = freq_index.shape[1]
        diagonal = iota((freqs, freqs), 0) == iota((freqs, freqs), 1)
        column = jnp.sum(
            jnp.where(diagonal, freq_index[...].astype(F32), 0.0), axis=1, keepdims=True
        ).astype(jnp.int32)
        phases = lax.rem(column * iota((freqs, length), 1), length)
        angles = phases.astype(F32) * jnp.float32(2.0 * math.pi / length)
        table[:freqs] = jnp.cos(angles).astype(BF16)
        table[freqs:] = (-jnp.sin(angles)).astype(BF16)

    with jax.named_scope("mask"):
        rblk, tiles = block_map.shape
        spread = one_hot(iota((tiles, points), 1) // (points // tiles) == iota((tiles, points), 0))
        colmask[...] = jnp.dot(block_map[...].astype(F32), spread, preferred_element_type=F32)
        load_rec.wait()
        load_src.wait()
        span = receivers // rblk

        @pl.loop(0, rblk, unroll=2)
        def _(b):
            row = jnp.broadcast_to(colmask[pl.ds(b, 1), :], (span, points)).astype(BF16)
            rows = pl.ds(pl.multiple_of(b * span, span), span)
            for c in range(2):
                masked[c, rows, :] = masked[c, rows, :] * row

    tb = BLOCK // SUB
    fb = tb // 2
    kb = tb // tsub
    swap_in = permutation(BLOCK, lambda row: row % tb * SUB + row // tb)
    swap_out = permutation(
        BLOCK, lambda row: row % SUB * tb + row // SUB % 2 * fb + row // (2 * SUB)
    )
    scale = 1.0 / math.sqrt(length)
    each = points // n
    pick[...] = one_hot(iota((n, points), 1) // each == iota((n, points), 0)).astype(BF16)
    fold[...] = one_hot(iota((points, LANES), 0) % each == iota((points, LANES), 1)).astype(BF16)
    back[...] = jnp.zeros_like(back)

    def transform(c):
        with jax.named_scope(f"wait_x{c}"):
            pltpu.make_async_copy(xbuf.at[c], xbuf.at[c], x_recv.at[c]).wait()

        with jax.named_scope(f"swap_in{c}"):
            @pl.loop(0, length // tb // 2, unroll=4)
            def _(b):
                both = [
                    xbuf[c, pl.ds((2 * b + h) * kb, kb)].reshape(BLOCK, LANES) for h in range(2)
                ]
                y = jnp.dot(swap_in, jnp.concatenate(both, axis=1), preferred_element_type=F32)
                y = y.astype(BF16).reshape(SUB, tb, 2 * LANES)
                for h in range(2):
                    rows = pl.ds(pl.multiple_of((2 * b + h) * tb, tb), tb)
                    for r in range(SUB):
                        xt[r // 2, rows, (r % 2) * LANES : (r % 2 + 1) * LANES] = y[
                            r, :, h * LANES : (h + 1) * LANES
                        ]

        with jax.named_scope(f"dft{c}"):
            for rp in range(SUB // 2):
                o = jnp.dot(table[...], xt[rp], preferred_element_type=F32) * scale
                o = o.astype(BF16)
                yb[2 * rp] = o[:, :LANES]
                yb[2 * rp + 1] = o[:, LANES:]

        with jax.named_scope(f"swap_out{c}"):
            def gathered(f0):
                parts = [yb[:, p * freqs + f0 : p * freqs + f0 + fb, :] for p in range(2)]
                return jnp.concatenate(parts, axis=1).reshape(BLOCK, LANES)

            for f0 in range(0, freqs, 2 * fb):
                both = [gathered(f0 + h * fb) for h in range(2)]
                y = jnp.dot(swap_out, jnp.concatenate(both, axis=1), preferred_element_type=F32)
                y = y.astype(BF16)
                for h in range(2):
                    spec[c, f0 + h * fb : f0 + (h + 1) * fb] = y[
                        :, h * LANES : (h + 1) * LANES
                    ].reshape(fb, 2, SUB, LANES)

        with jax.named_scope(f"scatter{c}"):
            def send_spectrum(j):
                pltpu.make_async_remote_copy(
                    src_ref=spec.at[c, j], dst_ref=pbuf.at[c, me],
                    send_sem=p_send, recv_sem=p_recv.at[c],
                    device_id={"freq": j}, device_id_type=MESH,
                ).start()

            peers.each(MIXED[0], send_spectrum)
            pbuf[c, me] = spec[c, me]

    def project(c):
        with jax.named_scope(f"wait_p{c}"):
            most = pbuf.at[c, pl.ds(0, n - 1)]
            pltpu.make_async_copy(most, most, p_recv.at[c]).wait()
        with jax.named_scope(f"project{c}"):
            rows = slice(c * per_chunk, (c + 1) * per_chunk)
            p0 = pbuf[c, :, 0].reshape(per_chunk, LANES)
            p1 = pbuf[c, :, 1].reshape(per_chunk, LANES)
            dims = (((0,), (0,)), ((), ()))
            back[...] += lax.dot_general(
                jnp.concatenate([p0, p1], axis=1), masked[0, rows, :], dims,
                preferred_element_type=F32,
            )
            back[...] += lax.dot_general(
                jnp.concatenate([p1, -p0], axis=1), masked[1, rows, :], dims,
                preferred_element_type=F32,
            )

    for c in range(CHUNKS):
        transform(c)
        if c > 0:
            project(c - 1)
    project(CHUNKS - 1)

    with jax.named_scope("image"):
        shots = src.shape[1]
        image = jnp.zeros((1, points), F32)
        for o in range(2):
            image += jnp.sum(
                src[o].astype(F32) * back[o * shots : (o + 1) * shots, :], axis=0, keepdims=True
            )
        rows = jnp.concatenate([pick[...] * p for p in three_parts(image)], axis=0)
        folded = jnp.dot(rows, fold[...], preferred_element_type=F32).reshape(3, n, LANES)
        istage[...] = (folded[0] + (folded[1] + folded[2])).reshape(n, 1, LANES)

    with jax.named_scope("reduce"):
        def send_image(j):
            pltpu.make_async_remote_copy(
                src_ref=istage.at[j], dst_ref=ibuf.at[me],
                send_sem=i_send, recv_sem=i_recv,
                device_id={"freq": j}, device_id_type=MESH,
            ).start()

        peers.each(FAR_FIRST, send_image)
        ibuf[me] = istage[me]
    with jax.named_scope("wait_i"):
        most = ibuf.at[pl.ds(0, n - 1)]
        pltpu.make_async_copy(most, most, i_recv).wait()
    with jax.named_scope("last"):
        out[...] = jnp.sum(ibuf[...], axis=0)[:, : points // n]

        for c in range(CHUNKS):
            most = xbuf.at[c, pl.ds(0, n - 1)]
            pltpu.make_async_copy(most, most, x_send).wait()
            most = pbuf.at[c, pl.ds(0, n - 1)]
            pltpu.make_async_copy(most, most, p_send).wait()
        most = ibuf.at[pl.ds(0, n - 1)]
        pltpu.make_async_copy(most, most, i_send).wait()


def body(traces, freq_index, block_map, green_rec, green_src):
    n = lax.axis_size("freq")
    tsub, receivers, shots = traces.shape
    length = tsub * n
    points = green_rec.shape[3]
    fcs = 2 * freq_index.shape[0]
    per = receivers // CHUNKS
    assert freq_index.shape[0] == n == SIDE * SIDE * CORES and per == n * SUB and shots == LANES
    any_spec = pl.BlockSpec(memory_space=pl.ANY)
    vmem = pl.BlockSpec(memory_space=pltpu.VMEM)
    dma = pltpu.SemaphoreType.DMA
    out = pl.pallas_call(
        functools.partial(kernel, n),
        out_shape=jax.ShapeDtypeStruct((1, points // n), F32),
        in_specs=[any_spec] * 5,
        out_specs=vmem,
        scratch_shapes=[
            pltpu.VMEM((1, n), jnp.int32),
            pltpu.VMEM(block_map.shape, jnp.int32),
            pltpu.VMEM((fcs, length), BF16),
            pltpu.VMEM((CHUNKS, n, tsub, SUB, LANES), BF16),
            pltpu.VMEM((SUB // 2, length, 2 * LANES), BF16),
            pltpu.VMEM((SUB, fcs, LANES), BF16),
            pltpu.VMEM((CHUNKS, n, 2, SUB, LANES), BF16),
            pltpu.VMEM((CHUNKS, n, 2, SUB, LANES), BF16),
            pltpu.VMEM((2, receivers, points), BF16),
            pltpu.VMEM((block_map.shape[0], points), F32),
            pltpu.VMEM((2, shots, points), BF16),
            pltpu.VMEM((2 * shots, points), F32),
            pltpu.VMEM((n, points), BF16),
            pltpu.VMEM((points, LANES), BF16),
            pltpu.VMEM((n, 1, LANES), F32),
            pltpu.VMEM((n, 1, LANES), F32),
            dma, dma((CHUNKS,)), dma, dma((CHUNKS,)), dma, dma, dma, dma, dma, dma,
            pltpu.SemaphoreType.REGULAR, pltpu.SemaphoreType.REGULAR,
        ],
        compiler_params=pltpu.CompilerParams(
            collective_id=0, has_side_effects=True, vmem_limit_bytes=60 * 2**20
        ),
    )(traces, freq_index[None], block_map, green_rec[0], green_src[0])
    return out[0]


def solution(mesh):
    placed = (
        P("freq", None, "groups"),
        P(),
        P(),
        P("freq", None, None, "groups"),
        P("freq", None, None, "groups"),
    )
    return jax.shard_map(
        body, mesh=mesh, in_specs=placed, out_specs=P(("groups", "freq")), check_vma=False
    )
```

```python
import functools
import math

import jax
import jax.numpy as jnp
from jax import lax
from jax.experimental import pallas as pl
from jax.experimental.pallas import tpu as pltpu
from jax.sharding import PartitionSpec as P

MESH = pl.DeviceIdType.MESH
BF16, F32 = jnp.bfloat16, jnp.float32
CHUNKS = 2
SUB = 8
LANES = 128
SIDE, CORES = 8, 2
STEPS = ((SIDE // 2) ** 2 - 1) * CORES
MIXED = ((17, 8), (19, 23))
FAR_FIRST = (STEPS - 1, 23)
BLOCK = 256
ROOT, AIDE = 0, 1
UNROLL = 3


def iota(shape, dim):
    return lax.broadcasted_iota(jnp.int32, shape, dim)


def one_hot(pred):
    return jnp.where(pred, 1.0, 0.0).astype(F32)


def permutation(size, source):
    row, col = iota((size, size), 0), iota((size, size), 1)
    return one_hot(source(row) == col).astype(BF16)


def turned(dx, dy, times):
    for _ in range(times):
        dx, dy = -dy, dx
    return dx, dy


class Peers:
    def __init__(self, me):
        self.core, self.y, self.x = me & (CORES - 1), (me // CORES) & (SIDE - 1), me // (CORES * SIDE)

    def at(self, dx, dy, dc):
        chip = ((self.x + dx) & (SIDE - 1)) * SIDE + ((self.y + dy) & (SIDE - 1))
        return chip * CORES + ((self.core + dc) & (CORES - 1))

    def opposite(self, send):
        half = SIDE // 2
        for dx, dy in ((half, half), (half, 0), (0, half)):
            for dc in range(CORES):
                send(self.at(dx, dy, dc))

    def turns(self, i, order, send):
        half = SIDE // 2
        stride, first = order
        e = (i * stride + first) % STEPS
        k, dc = e // CORES, e & (CORES - 1)
        a, b = 1 + (k & (half - 1)), (k // half + 1) & (half - 1)
        for times in range(4):
            dx, dy = turned(a, b, times)
            send(self.at(dx, dy, dc))

    def partner(self, send):
        for dc in range(1, CORES):
            send(self.at(0, 0, dc))

    def each(self, order, send):
        self.opposite(send)

        @pl.loop(0, STEPS, unroll=UNROLL)
        def _(i):
            self.turns(i, order, send)

        self.partner(send)


def three_parts(a):
    parts = []
    for _ in range(3):
        parts.append(a.astype(BF16))
        a = a - parts[-1].astype(F32)
    return parts


def kernel(
    n, traces, freq_hbm, map_hbm, green_rec, green_src, out,
    freq_index, block_map, table, xbuf, xt, yb, spec, pbuf, masked, colmask, src, back, pick, fold, istage, ibuf,
    x_send, x_recv, p_send, p_recv, i_send, i_recv, g_sem, s_sem, f_sem, m_sem, ready, root_in,
):
    me = lax.axis_index("freq")
    tsub, receivers, _ = traces.shape
    length = n * tsub
    points = green_rec.shape[2]
    per_chunk = receivers // CHUNKS

    barrier = pltpu.get_barrier_semaphore()

    def greet(j):
        pl.semaphore_signal(barrier, inc=1, device_id={"freq": j}, device_id_type=MESH)

    peers = Peers(me)

    @pl.when(me == ROOT)
    def _():
        greet(AIDE)

    @pl.when(me != ROOT)
    def _():
        peers.each(FAR_FIRST, lambda j: pl.when(j > AIDE)(lambda: greet(j)))

    load_rec = pltpu.make_async_copy(green_rec, masked, g_sem)
    load_src = pltpu.make_async_copy(green_src, src, s_sem)

    def block_of(c, j):
        start = pl.multiple_of(c * per_chunk + j * SUB, SUB)
        return traces.at[:, pl.ds(start, SUB), :]

    own = [
        pltpu.make_async_copy(block_of(c, me), xbuf.at[c, me], x_recv.at[c]) for c in range(CHUNKS)
    ]
    small = [
        pltpu.make_async_copy(freq_hbm, freq_index, f_sem),
        pltpu.make_async_copy(map_hbm, block_map, m_sem),
    ]
    for copy in [*own, *small, load_rec, load_src]:
        copy.start()

    def tell(semaphore, j):
        pl.semaphore_signal(semaphore, inc=1, device_id={"freq": j}, device_id_type=MESH)

    with jax.named_scope("barrier"):
        @pl.when(me > AIDE)
        def _():
            pl.semaphore_wait(barrier, n - 2)

        @pl.when(me == AIDE + 1)
        def _():
            tell(ready, AIDE)

        @pl.when(me <= AIDE)
        def _():
            pl.semaphore_wait(ready, 1)

    def send_block(c, j):
        pltpu.make_async_remote_copy(
            src_ref=block_of(c, j), dst_ref=xbuf.at[c, me],
            send_sem=x_send, recv_sem=x_recv.at[c],
            device_id={"freq": j}, device_id_type=MESH,
        ).start()

    def early(j):
        pl.when(j != ROOT)(lambda: send_block(0, j))

    def late(j):
        pl.when(j == ROOT)(lambda: send_block(0, j))

    split = STEPS * 2 // 5
    with jax.named_scope("send_early"):
        peers.opposite(early)

        @pl.loop(0, split, unroll=UNROLL)
        def _(i):
            peers.turns(i, MIXED[0], early)

    with jax.named_scope("root"):
        @pl.when(me == AIDE)
        def _():
            pl.semaphore_wait(barrier, 1)
            tell(ready, ROOT)
            peers.each(FAR_FIRST, lambda j: pl.when(j != ROOT)(lambda: tell(root_in, j)))

        @pl.when(me > AIDE)
        def _():
            pl.semaphore_wait(root_in, 1)

    with jax.named_scope("send"):
        peers.opposite(late)

        @pl.loop(0, split)
        def _(i):
            peers.turns(i, MIXED[0], late)

        @pl.loop(split, STEPS, unroll=UNROLL)
        def _(i):
            peers.turns(i, MIXED[0], lambda j: send_block(0, j))

        peers.partner(lambda j: send_block(0, j))
        for c in range(1, CHUNKS):
            peers.each(MIXED[c], lambda j, c=c: send_block(c, j))

    with jax.named_scope("table"):
        for copy in small:
            copy.wait()
        freqs = freq_index.shape[1]
        diagonal = iota((freqs, freqs), 0) == iota((freqs, freqs), 1)
        column = jnp.sum(
            jnp.where(diagonal, freq_index[...].astype(F32), 0.0), axis=1, keepdims=True
        ).astype(jnp.int32)
        phases = lax.rem(column * iota((freqs, length), 1), length)
        angles = phases.astype(F32) * jnp.float32(2.0 * math.pi / length)
        table[:freqs] = jnp.cos(angles).astype(BF16)
        table[freqs:] = (-jnp.sin(angles)).astype(BF16)

    with jax.named_scope("mask"):
        rblk, tiles = block_map.shape
        spread = one_hot(iota((tiles, points), 1) // (points // tiles) == iota((tiles, points), 0))
        colmask[...] = jnp.dot(block_map[...].astype(F32), spread, preferred_element_type=F32)
        load_rec.wait()
        load_src.wait()
        span = receivers // rblk

        @pl.loop(0, rblk, unroll=2)
        def _(b):
            row = jnp.broadcast_to(colmask[pl.ds(b, 1), :], (span, points)).astype(BF16)
            rows = pl.ds(pl.multiple_of(b * span, span), span)
            for c in range(2):
                masked[c, rows, :] = masked[c, rows, :] * row

    tb = BLOCK // SUB
    fb = tb // 2
    kb = tb // tsub
    swap_in = permutation(BLOCK, lambda row: row % tb * SUB + row // tb)
    swap_out = permutation(
        BLOCK, lambda row: row % SUB * tb + row // SUB % 2 * fb + row // (2 * SUB)
    )
    scale = 1.0 / math.sqrt(length)
    each = points // n
    pick[...] = one_hot(iota((n, points), 1) // each == iota((n, points), 0)).astype(BF16)
    fold[...] = one_hot(iota((points, LANES), 0) % each == iota((points, LANES), 1)).astype(BF16)
    back[...] = jnp.zeros_like(back)

    def transform(c):
        with jax.named_scope(f"wait_x{c}"):
            pltpu.make_async_copy(xbuf.at[c], xbuf.at[c], x_recv.at[c]).wait()

        with jax.named_scope(f"swap_in{c}"):
            @pl.loop(0, length // tb // 2, unroll=4)
            def _(b):
                both = [
                    xbuf[c, pl.ds((2 * b + h) * kb, kb)].reshape(BLOCK, LANES) for h in range(2)
                ]
                y = jnp.dot(swap_in, jnp.concatenate(both, axis=1), preferred_element_type=F32)
                y = y.astype(BF16).reshape(SUB, tb, 2 * LANES)
                for h in range(2):
                    rows = pl.ds(pl.multiple_of((2 * b + h) * tb, tb), tb)
                    for r in range(SUB):
                        xt[r // 2, rows, (r % 2) * LANES : (r % 2 + 1) * LANES] = y[
                            r, :, h * LANES : (h + 1) * LANES
                        ]

        with jax.named_scope(f"dft{c}"):
            for rp in range(SUB // 2):
                o = jnp.dot(table[...], xt[rp], preferred_element_type=F32) * scale
                o = o.astype(BF16)
                yb[2 * rp] = o[:, :LANES]
                yb[2 * rp + 1] = o[:, LANES:]

        with jax.named_scope(f"swap_out{c}"):
            def gathered(f0):
                parts = [yb[:, p * freqs + f0 : p * freqs + f0 + fb, :] for p in range(2)]
                return jnp.concatenate(parts, axis=1).reshape(BLOCK, LANES)

            for f0 in range(0, freqs, 2 * fb):
                both = [gathered(f0 + h * fb) for h in range(2)]
                y = jnp.dot(swap_out, jnp.concatenate(both, axis=1), preferred_element_type=F32)
                y = y.astype(BF16)
                for h in range(2):
                    spec[c, f0 + h * fb : f0 + (h + 1) * fb] = y[
                        :, h * LANES : (h + 1) * LANES
                    ].reshape(fb, 2, SUB, LANES)

        with jax.named_scope(f"scatter{c}"):
            def send_spectrum(j):
                pltpu.make_async_remote_copy(
                    src_ref=spec.at[c, j], dst_ref=pbuf.at[c, me],
                    send_sem=p_send, recv_sem=p_recv.at[c],
                    device_id={"freq": j}, device_id_type=MESH,
                ).start()

            peers.each(MIXED[0], send_spectrum)
            pbuf[c, me] = spec[c, me]

    def project(c):
        with jax.named_scope(f"wait_p{c}"):
            most = pbuf.at[c, pl.ds(0, n - 1)]
            pltpu.make_async_copy(most, most, p_recv.at[c]).wait()
        with jax.named_scope(f"project{c}"):
            rows = slice(c * per_chunk, (c + 1) * per_chunk)
            p0 = pbuf[c, :, 0].reshape(per_chunk, LANES)
            p1 = pbuf[c, :, 1].reshape(per_chunk, LANES)
            dims = (((0,), (0,)), ((), ()))
            back[...] += lax.dot_general(
                jnp.concatenate([p0, p1], axis=1), masked[0, rows, :], dims,
                preferred_element_type=F32,
            )
            back[...] += lax.dot_general(
                jnp.concatenate([p1, -p0], axis=1), masked[1, rows, :], dims,
                preferred_element_type=F32,
            )

    for c in range(CHUNKS):
        transform(c)
        if c > 0:
            project(c - 1)
    project(CHUNKS - 1)

    with jax.named_scope("image"):
        shots = src.shape[1]
        image = jnp.zeros((1, points), F32)
        for o in range(2):
            image += jnp.sum(
                src[o].astype(F32) * back[o * shots : (o + 1) * shots, :], axis=0, keepdims=True
            )
        rows = jnp.concatenate([pick[...] * p for p in three_parts(image)], axis=0)
        folded = jnp.dot(rows, fold[...], preferred_element_type=F32).reshape(3, n, LANES)
        istage[...] = (folded[0] + (folded[1] + folded[2])).reshape(n, 1, LANES)

    with jax.named_scope("reduce"):
        def send_image(j):
            pltpu.make_async_remote_copy(
                src_ref=istage.at[j], dst_ref=ibuf.at[me],
                send_sem=i_send, recv_sem=i_recv,
                device_id={"freq": j}, device_id_type=MESH,
            ).start()

        peers.each(FAR_FIRST, send_image)
        ibuf[me] = istage[me]
    with jax.named_scope("wait_i"):
        most = ibuf.at[pl.ds(0, n - 1)]
        pltpu.make_async_copy(most, most, i_recv).wait()
    with jax.named_scope("last"):
        out[...] = jnp.sum(ibuf[...], axis=0)[:, : points // n]

        for c in range(CHUNKS):
            most = xbuf.at[c, pl.ds(0, n - 1)]
            pltpu.make_async_copy(most, most, x_send).wait()
            most = pbuf.at[c, pl.ds(0, n - 1)]
            pltpu.make_async_copy(most, most, p_send).wait()
        most = ibuf.at[pl.ds(0, n - 1)]
        pltpu.make_async_copy(most, most, i_send).wait()


def body(traces, freq_index, block_map, green_rec, green_src):
    n = lax.axis_size("freq")
    tsub, receivers, shots = traces.shape
    length = tsub * n
    points = green_rec.shape[3]
    fcs = 2 * freq_index.shape[0]
    per = receivers // CHUNKS
    assert freq_index.shape[0] == n == SIDE * SIDE * CORES and per == n * SUB and shots == LANES
    any_spec = pl.BlockSpec(memory_space=pl.ANY)
    vmem = pl.BlockSpec(memory_space=pltpu.VMEM)
    dma = pltpu.SemaphoreType.DMA
    out = pl.pallas_call(
        functools.partial(kernel, n),
        out_shape=jax.ShapeDtypeStruct((1, points // n), F32),
        in_specs=[any_spec] * 5,
        out_specs=vmem,
        scratch_shapes=[
            pltpu.VMEM((1, n), jnp.int32),
            pltpu.VMEM(block_map.shape, jnp.int32),
            pltpu.VMEM((fcs, length), BF16),
            pltpu.VMEM((CHUNKS, n, tsub, SUB, LANES), BF16),
            pltpu.VMEM((SUB // 2, length, 2 * LANES), BF16),
            pltpu.VMEM((SUB, fcs, LANES), BF16),
            pltpu.VMEM((CHUNKS, n, 2, SUB, LANES), BF16),
            pltpu.VMEM((CHUNKS, n, 2, SUB, LANES), BF16),
            pltpu.VMEM((2, receivers, points), BF16),
            pltpu.VMEM((block_map.shape[0], points), F32),
            pltpu.VMEM((2, shots, points), BF16),
            pltpu.VMEM((2 * shots, points), F32),
            pltpu.VMEM((n, points), BF16),
            pltpu.VMEM((points, LANES), BF16),
            pltpu.VMEM((n, 1, LANES), F32),
            pltpu.VMEM((n, 1, LANES), F32),
            dma, dma((CHUNKS,)), dma, dma((CHUNKS,)), dma, dma, dma, dma, dma, dma,
            pltpu.SemaphoreType.REGULAR, pltpu.SemaphoreType.REGULAR,
        ],
        compiler_params=pltpu.CompilerParams(
            collective_id=0, has_side_effects=True, vmem_limit_bytes=60 * 2**20
        ),
    )(traces, freq_index[None], block_map, green_rec[0], green_src[0])
    return out[0]


def solution(mesh):
    placed = (
        P("freq", None, "groups"),
        P(),
        P(),
        P("freq", None, None, "groups"),
        P("freq", None, None, "groups"),
    )
    return jax.shard_map(
        body, mesh=mesh, in_specs=placed, out_specs=P(("groups", "freq")), check_vma=False
    )
```
